256 devices in a mesh: worker: 16 (over y, x_hi, core), mp: 16 (over z, x_lo).
Axes of the slice: x: 4 (x_hi: 2, x_lo: 2; x = x_hi * 2 + x_lo), y: 4, z: 8, core: 2. Of those that a mesh axis runs over, the one named last changes fastest.
Arguments:
- gradients: float32 [16, 8388608], P('worker', 'mp'), may hold values from -100 to 100
- neighbours: int32 [16, 11], replicated, may hold values from 0 to 15, as said below
- winner: int32 [1], replicated, may hold values from 0 to 15
Outputs:
- scores: float32 [16], replicated
- aggregate: float32 [8388608], P(('mp', 'worker'))
The draws below stay inside these ranges and needn't reach their ends.
Inputs may be any that keep to these rules, and one draw needn't show every extreme that they name: `neighbours`: row i lists 11 different workers, none of them equal to i.
All inputs are finite; a program needn't handle non-finite values.
Results may differ from the reference program's by a relative error of at most 0.0003.
Values may be sent and summed in bfloat16 or wider, within the bound.
A program may use at most 64 MiB of HBM per device.

```python
import math
import jax
import jax.numpy as jnp
from jax import lax

FAULTY = 3
WORKERS = 16
NBR = 11
PARAMS = 8388608


def draw_gradients(key, part):
    keys = jax.random.split(jax.random.fold_in(key, 11), 10)
    noise = jnp.clip(jax.random.normal(keys[0], (WORKERS, PARAMS), jnp.float32), -6.0, 6.0)
    position = jnp.arange(PARAMS, dtype=jnp.float32) / jnp.float32(PARAMS)
    scales = jnp.exp(jax.random.uniform(keys[1], (WORKERS, 1), jnp.float32, math.log(0.5), math.log(2.0)))
    column = 0.5 * jnp.exp(math.log(3.0) * position)[None, :]
    values = scales * column * noise
    loadings = jax.random.uniform(keys[8], (WORKERS, 4), jnp.float32, -1.0, 1.0)
    shared = jnp.clip(jax.random.normal(keys[9], (4, PARAMS), jnp.float32), -6.0, 6.0)
    for factor in range(4):
        values = values + column * loadings[:, factor:factor + 1] * shared[factor][None, :]
    ranking = jax.random.permutation(keys[4], WORKERS)
    faulty = (ranking < FAULTY).astype(jnp.float32)[:, None]
    sparse = (jax.random.uniform(keys[5], (WORKERS, PARAMS), jnp.float32) < 1.0 / 4096.0).astype(jnp.float32)
    size = jax.random.uniform(keys[6], (WORKERS, PARAMS), jnp.float32, 20.0, 40.0)
    sign = jnp.where(jax.random.uniform(keys[7], (WORKERS, PARAMS), jnp.float32) < 0.5, -1.0, 1.0)
    values = values + faulty * sparse * sign * size * column
    return jnp.clip(values, -100.0, 100.0).astype(jnp.float32)


def draw_neighbours(key, part):
    keys = jax.random.split(jax.random.fold_in(key, 23), WORKERS)
    orders = jax.vmap(lambda single: jax.random.permutation(single, WORKERS - 1))(keys)[:, :NBR]
    orders = orders.astype(jnp.int32)
    own_index = jnp.arange(WORKERS, dtype=jnp.int32)[:, None]
    return (orders + (orders >= own_index).astype(jnp.int32)).astype(jnp.int32)


def setup_inputs(seed: int = 0) -> dict:
    streams_of = jax.random.split(jax.random.key(seed), 4)
    return {
        "gradients": draw_gradients(jax.random.fold_in(streams_of[3], 71), 0),
        "neighbours": draw_neighbours(jax.random.fold_in(streams_of[3], 71), 0),
        "winner": jax.random.randint(streams_of[2], (1,), 0, WORKERS).astype(jnp.int32),
    }


def reference(gradients, neighbours, winner):
    rounded = gradients.astype(jnp.bfloat16)
    gram_matrix = jnp.dot(rounded, rounded.T, preferred_element_type=jnp.float32)
    squares = jnp.diagonal(gram_matrix)
    distance = squares[:, None] + squares[None, :] - 2.0 * gram_matrix
    chosen = jnp.take_along_axis(distance, neighbours, axis=1)
    scores = jnp.sum(chosen, axis=1) / jnp.float32(NBR * PARAMS)
    aggregate = lax.dynamic_index_in_dim(gradients, winner[0], 0, keepdims=False)
    return (scores, aggregate)
```

```python
import functools

import jax
import jax.numpy as jnp
from jax import lax
from jax.experimental import pallas as pl
from jax.experimental.pallas import tpu as pltpu
from jax.sharding import Mesh
from jax.sharding import PartitionSpec as P

AXES = ("y", "xh", "c", "z", "xl")
WORKER = ("y", "xh", "c")
MP = ("z", "xl")
MP_WORKER = ("z", "xl", "y", "xh", "c")
MESH = pl.DeviceIdType.MESH

WORKERS = 16
ROWS = 256
HALF = ROWS // 2
LANES = 128

CHIPS = [(2, 2), (2, 0), (0, 2), (2, 1), (0, 1), (2, 3), (0, 3)]
PEERS = [(dx, dy, 0, c) for dx, dy in CHIPS for c in (0, 1)] + [(0, 0, 0, 1)]
LINE = [(0, 0, dz, 0) for dz in (4, 3, 5, 2, 6, 1, 7)]
PLANE = [
    (dx, dy, 0, c)
    for dx, dy in sorted(
        ((a, b) for a in range(4) for b in range(4)),
        key=lambda p: -(min(p[0], 4 - p[0]) + min(p[1], 4 - p[1])),
    )
    for c in (0, 1)
    if (dx, dy, c) != (0, 0, 0)
]


def place():
    x = lax.axis_index("xh") * 2 + lax.axis_index("xl")
    return x, lax.axis_index("y"), lax.axis_index("z"), lax.axis_index("c")


def at_offset(offset):
    x, y, z, c = (
        lax.rem(own + step, size) for own, step, size in zip(place(), offset, (4, 4, 8, 2))
    )
    return x, y, z, c


def device(offset):
    x, y, z, c = at_offset(offset)
    return {"y": y, "xh": x // 2, "c": c, "z": z, "xl": lax.rem(x, 2)}


def chip_index(offset):
    x, y, _, _ = at_offset(offset)
    return y * 2 + x // 2


def worker_index(offset):
    return chip_index(offset) * 2 + at_offset(offset)[3]


def send(src, dst, send_sem, recv_sem, offset):
    copy = pltpu.make_async_remote_copy(
        src_ref=src,
        dst_ref=dst,
        send_sem=send_sem,
        recv_sem=recv_sem,
        device_id=device(offset),
        device_id_type=MESH,
    )
    copy.start()
    return copy


def wait_bytes(ref, sem):
    pltpu.make_async_copy(ref, ref, sem).wait()


def kernel(
    total_entries,
    winner_ref,
    neighbours_ref,
    gradients_ref,
    scores_ref,
    aggregate_ref,
    full,
    hi,
    lo,
    lo_away,
    lo_mine,
    lo_got,
    got,
    gram,
    line_src,
    line_got,
    plane_src,
    plane_got,
    load_sem,
    hi_send,
    hi_recv,
    lo_send,
    lo_recv,
    sum_send,
    sum_recv,
):
    own_core = lax.axis_index("c")
    own_chip = chip_index((0, 0, 0, 0))
    own = worker_index((0, 0, 0, 0))
    winner = winner_ref[0]

    order = PEERS + [(0, 0, 0, 0)]
    loads = []
    for slot, offset in enumerate(order):
        rows = pl.ds(pl.multiple_of(worker_index(offset) * ROWS, ROWS), ROWS)
        load = pltpu.make_async_copy(gradients_ref.at[rows], full.at[slot], load_sem.at[slot])
        load.start()
        loads.append(load)

    barrier = pltpu.get_barrier_semaphore()
    partners = LINE + PLANE
    for offset in partners:
        pl.semaphore_signal(barrier, inc=1, device_id=device(offset), device_id_type=MESH)

    for slot, offset in enumerate(order):
        loads[slot].wait()
        value = full[slot]
        high = value.astype(jnp.bfloat16)
        low = (value - high.astype(jnp.float32)).astype(jnp.bfloat16)
        if slot < len(PEERS):
            hi[slot] = high
        else:
            got[own] = high
        if offset[3] == 0:
            lo[own_core, chip_index(offset)] = low
        else:
            lo_away[chip_index(offset)] = low

    pl.semaphore_wait(barrier, len(partners))

    copies = []
    for half in range(2):
        rows = pl.ds(half * HALF, HALF)
        for slot, offset in enumerate(PEERS):
            copies.append(
                send(
                    hi.at[slot, rows],
                    got.at[own, rows],
                    hi_send.at[half],
                    hi_recv.at[half],
                    offset,
                )
            )
    swap = send(lo_away, lo.at[own_core], lo_send.at[0], lo_recv.at[0], (0, 0, 0, 1))

    row = lax.broadcasted_iota(jnp.int32, (WORKERS, ROWS), 0)
    column = lax.broadcasted_iota(jnp.int32, (WORKERS, ROWS), 1) // 16
    counts = jnp.zeros((WORKERS, ROWS), jnp.float32)
    number = neighbours_ref.shape[1]
    for entry in range(number):
        counts += (neighbours_ref[:, entry : entry + 1] == column).astype(jnp.float32)
    line_src[...] = jnp.zeros_like(line_src)

    swap.wait()
    lo_mine[...] = lo[lax.rem(winner, 2)]

    def product(half):
        parts = [
            got[:, pl.ds(half * HALF + step * 16, 16), :].reshape(ROWS, LANES)
            for step in range(HALF // 16)
        ]
        block = jnp.concatenate(parts, axis=1)
        return lax.dot_general(
            block, block, (((1,), (1,)), ((), ())), preferred_element_type=jnp.float32
        )

    wait_bytes(got.at[pl.ds(0, 15), pl.ds(0, HALF)], hi_recv.at[0])
    gram[...] = product(0)
    wait_bytes(got.at[pl.ds(0, 15), pl.ds(0, HALF)], hi_recv.at[1])

    for dx, dy in CHIPS:
        offset = (dx, dy, 0, 0)
        send(
            lo_mine.at[chip_index(offset)],
            lo_got.at[own_chip],
            lo_send.at[1],
            lo_recv.at[1],
            offset,
        )
    lo_got[own_chip] = lo_mine[own_chip]

    total = gram[...] + product(1)
    sublane = lax.broadcasted_iota(jnp.int32, (ROWS, ROWS), 0)
    lane = lax.broadcasted_iota(jnp.int32, (ROWS, ROWS), 1)
    total = jnp.where(lax.rem(sublane, 16) == lax.rem(lane, 16), total, 0.0)
    total = jnp.sum(total.reshape(WORKERS, 16, ROWS), axis=1)
    diagonal = jnp.where(row == column, total, 0.0)
    squares = jnp.sum(diagonal, axis=0, keepdims=True)
    own_counts = jnp.sum(counts, axis=1, keepdims=True) * (1.0 / 16.0)
    partial = counts * (squares - 2.0 * total) + own_counts * diagonal
    partial = lax.dot_general(
        jnp.ones((8, ROWS), jnp.float32),
        partial,
        (((1,), (1,)), ((), ())),
        precision=lax.Precision.HIGHEST,
        preferred_element_type=jnp.float32,
    )
    line_src[:, pl.ds(0, WORKERS)] = partial[0:1]

    for step, offset in enumerate(LINE):
        send(line_src, line_got.at[step], sum_send.at[0], sum_recv.at[0], offset)
    wait_bytes(line_got, sum_recv.at[0])
    plane_src[...] = line_src[...] + jnp.sum(line_got[...], axis=0)
    for step, offset in enumerate(PLANE):
        send(plane_src, plane_got.at[step], sum_send.at[1], sum_recv.at[1], offset)

    wait_bytes(lo_got.at[pl.ds(0, 7)], lo_recv.at[1])
    aggregate_ref[...] = got[winner].astype(jnp.float32) + lo_got[winner // 2].astype(jnp.float32)

    wait_bytes(plane_got, sum_recv.at[1])
    scores = (plane_src[...] + jnp.sum(plane_got[...], axis=0)) / jnp.float32(total_entries)
    scores_ref[...] = scores

    for half in range(2):
        wait_bytes(got.at[pl.ds(0, 15), pl.ds(0, HALF)], hi_send.at[half])
    wait_bytes(lo_got.at[pl.ds(0, 7)], lo_send.at[1])
    wait_bytes(line_got, sum_send.at[0])
    wait_bytes(plane_got, sum_send.at[1])


def body(gradients, neighbours, winner):
    length = gradients.shape[1]
    total_entries = neighbours.shape[1] * length * lax.axis_size(MP)
    bf16, f32 = jnp.bfloat16, jnp.float32
    scores, aggregate = pl.pallas_call(
        functools.partial(kernel, total_entries),
        out_shape=(
            jax.ShapeDtypeStruct((1, LANES), f32),
            jax.ShapeDtypeStruct((ROWS, LANES), f32),
        ),
        in_specs=[
            pl.BlockSpec(memory_space=pltpu.SMEM),
            pl.BlockSpec(memory_space=pltpu.VMEM),
            pl.BlockSpec(memory_space=pl.ANY),
        ],
        out_specs=(
            pl.BlockSpec(memory_space=pltpu.VMEM),
            pl.BlockSpec(memory_space=pltpu.VMEM),
        ),
        scratch_shapes=[
            pltpu.VMEM((16, ROWS, LANES), f32),
            pltpu.VMEM((15, ROWS, LANES), bf16),
            pltpu.VMEM((2, 8, ROWS, LANES), bf16),
            pltpu.VMEM((8, ROWS, LANES), bf16),
            pltpu.VMEM((8, ROWS, LANES), bf16),
            pltpu.VMEM((8, ROWS, LANES), bf16),
            pltpu.VMEM((16, ROWS, LANES), bf16),
            pltpu.VMEM((ROWS, ROWS), f32),
            pltpu.VMEM((1, LANES), f32),
            pltpu.VMEM((len(LINE), 1, LANES), f32),
            pltpu.VMEM((1, LANES), f32),
            pltpu.VMEM((len(PLANE), 1, LANES), f32),
            pltpu.SemaphoreType.DMA((16,)),
            pltpu.SemaphoreType.DMA((2,)),
            pltpu.SemaphoreType.DMA((2,)),
            pltpu.SemaphoreType.DMA((2,)),
            pltpu.SemaphoreType.DMA((2,)),
            pltpu.SemaphoreType.DMA((2,)),
            pltpu.SemaphoreType.DMA((2,)),
        ],
        compiler_params=pltpu.CompilerParams(collective_id=0, has_side_effects=True),
        name="krum",
    )(winner, neighbours, gradients.reshape(length // LANES, LANES))
    return scores[0, :WORKERS], aggregate.reshape(-1)


def solution(mesh):
    split = Mesh(mesh.devices.reshape(4, 2, 2, 8, 2), AXES)
    in_specs = (P(WORKER, MP), P(), P())
    out_specs = (P(), P(MP_WORKER))
    return jax.shard_map(body, mesh=split, in_specs=in_specs, out_specs=out_specs, check_vma=False)
```

```python
import functools

import jax
import jax.numpy as jnp
from jax import lax
from jax.experimental import pallas as pl
from jax.experimental.pallas import tpu as pltpu
from jax.sharding import Mesh
from jax.sharding import PartitionSpec as P

AXES = ("y", "xh", "c", "z", "xl")
WORKER = ("y", "xh", "c")
MP = ("z", "xl")
MP_WORKER = ("z", "xl", "y", "xh", "c")
MESH = pl.DeviceIdType.MESH

WORKERS = 16
ROWS = 256
HALF = ROWS // 2
LANES = 128

CHIPS = [(2, 2), (2, 0), (0, 2), (2, 1), (0, 1), (2, 3), (0, 3)]
PEERS = [(dx, dy, 0, c) for dx, dy in CHIPS for c in (0, 1)] + [(0, 0, 0, 1)]
LINE = [(0, 0, dz, 0) for dz in (4, 3, 5, 2, 6, 1, 7)]
PLANE = [
    (dx, dy, 0, c)
    for dx, dy in sorted(
        ((a, b) for a in range(4) for b in range(4)),
        key=lambda p: -(min(p[0], 4 - p[0]) + min(p[1], 4 - p[1])),
    )
    for c in (0, 1)
    if (dx, dy, c) != (0, 0, 0)
]


def place():
    x = lax.axis_index("xh") * 2 + lax.axis_index("xl")
    return x, lax.axis_index("y"), lax.axis_index("z"), lax.axis_index("c")


def at_offset(offset):
    x, y, z, c = (
        lax.rem(own + step, size) for own, step, size in zip(place(), offset, (4, 4, 8, 2))
    )
    return x, y, z, c


def device(offset):
    x, y, z, c = at_offset(offset)
    return {"y": y, "xh": x // 2, "c": c, "z": z, "xl": lax.rem(x, 2)}


def chip_index(offset):
    x, y, _, _ = at_offset(offset)
    return y * 2 + x // 2


def worker_index(offset):
    return chip_index(offset) * 2 + at_offset(offset)[3]


def send(src, dst, send_sem, recv_sem, offset):
    copy = pltpu.make_async_remote_copy(
        src_ref=src,
        dst_ref=dst,
        send_sem=send_sem,
        recv_sem=recv_sem,
        device_id=device(offset),
        device_id_type=MESH,
    )
    copy.start()
    return copy


def wait_bytes(ref, sem):
    pltpu.make_async_copy(ref, ref, sem).wait()


def kernel(
    total_entries,
    winner_ref,
    neighbours_hbm,
    gradients_ref,
    scores_ref,
    aggregate_ref,
    full,
    hi,
    lo,
    lo_away,
    lo_mine,
    lo_got,
    got,
    gram,
    line_src,
    line_got,
    plane_src,
    plane_got,
    neighbours_ref,
    load_sem,
    hi_send,
    hi_recv,
    lo_send,
    lo_recv,
    sum_send,
    sum_recv,
):
    own_core = lax.axis_index("c")
    own_chip = chip_index((0, 0, 0, 0))
    own = worker_index((0, 0, 0, 0))
    fetch = pltpu.make_async_copy(neighbours_hbm, neighbours_ref, load_sem.at[16])
    order = PEERS + [(0, 0, 0, 0)]
    loads = []
    for slot, offset in enumerate(order):
        rows = pl.ds(pl.multiple_of(worker_index(offset) * ROWS, ROWS), ROWS)
        load = pltpu.make_async_copy(gradients_ref.at[rows], full.at[slot], load_sem.at[slot])
        load.start()
        loads.append(load)
    fetch.start()

    barrier = pltpu.get_barrier_semaphore()
    partners = LINE + PLANE
    for offset in partners:
        pl.semaphore_signal(barrier, inc=1, device_id=device(offset), device_id_type=MESH)

    for slot, offset in enumerate(order):
        loads[slot].wait()
        value = full[slot]
        high = value.astype(jnp.bfloat16)
        low = (value - high.astype(jnp.float32)).astype(jnp.bfloat16)
        if slot < len(PEERS):
            hi[slot] = high
        else:
            got[own] = high
        if offset[3] == 0:
            lo[own_core, chip_index(offset)] = low
        else:
            lo_away[chip_index(offset)] = low

    pl.semaphore_wait(barrier, len(partners))

    copies = []
    for half in range(2):
        rows = pl.ds(half * HALF, HALF)
        for slot, offset in enumerate(PEERS):
            copies.append(
                send(
                    hi.at[slot, rows],
                    got.at[own, rows],
                    hi_send.at[half],
                    hi_recv.at[half],
                    offset,
                )
            )
    swap = send(lo_away, lo.at[own_core], lo_send.at[0], lo_recv.at[0], (0, 0, 0, 1))

    fetch.wait()
    winner = winner_ref[0]
    row = lax.broadcasted_iota(jnp.int32, (WORKERS, ROWS), 0)
    column = lax.broadcasted_iota(jnp.int32, (WORKERS, ROWS), 1) // 16
    counts = jnp.zeros((WORKERS, ROWS), jnp.float32)
    number = neighbours_ref.shape[1]
    for entry in range(number):
        counts += (neighbours_ref[:, entry : entry + 1] == column).astype(jnp.float32)
    line_src[...] = jnp.zeros_like(line_src)

    swap.wait()
    lo_mine[...] = lo[lax.rem(winner, 2)]

    def product(half):
        parts = [
            got[:, pl.ds(half * HALF + step * 16, 16), :].reshape(ROWS, LANES)
            for step in range(HALF // 16)
        ]
        block = jnp.concatenate(parts, axis=1)
        return lax.dot_general(
            block, block, (((1,), (1,)), ((), ())), preferred_element_type=jnp.float32
        )

    wait_bytes(got.at[pl.ds(0, 15), pl.ds(0, HALF)], hi_recv.at[0])
    gram[...] = product(0)
    wait_bytes(got.at[pl.ds(0, 15), pl.ds(0, HALF)], hi_recv.at[1])

    for dx, dy in CHIPS:
        offset = (dx, dy, 0, 0)
        send(
            lo_mine.at[chip_index(offset)],
            lo_got.at[own_chip],
            lo_send.at[1],
            lo_recv.at[1],
            offset,
        )
    lo_got[own_chip] = lo_mine[own_chip]

    total = gram[...] + product(1)
    sublane = lax.broadcasted_iota(jnp.int32, (ROWS, ROWS), 0)
    lane = lax.broadcasted_iota(jnp.int32, (ROWS, ROWS), 1)
    total = jnp.where(lax.rem(sublane, 16) == lax.rem(lane, 16), total, 0.0)
    total = jnp.sum(total.reshape(WORKERS, 16, ROWS), axis=1)
    diagonal = jnp.where(row == column, total, 0.0)
    squares = jnp.sum(diagonal, axis=0, keepdims=True)
    own_counts = jnp.sum(counts, axis=1, keepdims=True) * (1.0 / 16.0)
    partial = counts * (squares - 2.0 * total) + own_counts * diagonal
    partial = lax.dot_general(
        jnp.ones((8, ROWS), jnp.float32),
        partial,
        (((1,), (1,)), ((), ())),
        precision=lax.Precision.HIGHEST,
        preferred_element_type=jnp.float32,
    )
    line_src[:, pl.ds(0, WORKERS)] = partial[0:1]

    for step, offset in enumerate(LINE):
        send(line_src, line_got.at[step], sum_send.at[0], sum_recv.at[0], offset)
    wait_bytes(line_got, sum_recv.at[0])
    plane_src[...] = line_src[...] + jnp.sum(line_got[...], axis=0)
    for step, offset in enumerate(PLANE):
        send(plane_src, plane_got.at[step], sum_send.at[1], sum_recv.at[1], offset)

    wait_bytes(lo_got.at[pl.ds(0, 7)], lo_recv.at[1])
    aggregate_ref[...] = got[winner].astype(jnp.float32) + lo_got[winner // 2].astype(jnp.float32)

    wait_bytes(plane_got, sum_recv.at[1])
    scores = (plane_src[...] + jnp.sum(plane_got[...], axis=0)) / jnp.float32(total_entries)
    scores_ref[...] = scores

    for half in range(2):
        wait_bytes(got.at[pl.ds(0, 15), pl.ds(0, HALF)], hi_send.at[half])
    wait_bytes(lo_got.at[pl.ds(0, 7)], lo_send.at[1])
    wait_bytes(line_got, sum_send.at[0])
    wait_bytes(plane_got, sum_send.at[1])


def finish(row_ref, block_ref, scores_ref, aggregate_ref, sem):
    copy = pltpu.make_async_copy(block_ref, aggregate_ref, sem)
    copy.start()
    scores_ref[...] = row_ref[0, :WORKERS]
    copy.wait()


def body(gradients, neighbours, winner):
    length = gradients.shape[1]
    total_entries = neighbours.shape[1] * length * lax.axis_size(MP)
    bf16, f32 = jnp.bfloat16, jnp.float32
    scores, aggregate = pl.pallas_call(
        functools.partial(kernel, total_entries),
        out_shape=(
            jax.ShapeDtypeStruct((1, LANES), f32),
            jax.ShapeDtypeStruct((ROWS, LANES), f32),
        ),
        in_specs=[
            pl.BlockSpec(memory_space=pltpu.SMEM),
            pl.BlockSpec(memory_space=pltpu.HBM),
            pl.BlockSpec(memory_space=pltpu.HBM),
        ],
        out_specs=(
            pl.BlockSpec(memory_space=pltpu.VMEM),
            pl.BlockSpec(memory_space=pltpu.VMEM),
        ),
        scratch_shapes=[
            pltpu.VMEM((16, ROWS, LANES), f32),
            pltpu.VMEM((15, ROWS, LANES), bf16),
            pltpu.VMEM((2, 8, ROWS, LANES), bf16),
            pltpu.VMEM((8, ROWS, LANES), bf16),
            pltpu.VMEM((8, ROWS, LANES), bf16),
            pltpu.VMEM((8, ROWS, LANES), bf16),
            pltpu.VMEM((16, ROWS, LANES), bf16),
            pltpu.VMEM((ROWS, ROWS), f32),
            pltpu.VMEM((1, LANES), f32),
            pltpu.VMEM((len(LINE), 1, LANES), f32),
            pltpu.VMEM((1, LANES), f32),
            pltpu.VMEM((len(PLANE), 1, LANES), f32),
            pltpu.VMEM(neighbours.shape, jnp.int32),
            pltpu.SemaphoreType.DMA((17,)),
            pltpu.SemaphoreType.DMA((2,)),
            pltpu.SemaphoreType.DMA((2,)),
            pltpu.SemaphoreType.DMA((2,)),
            pltpu.SemaphoreType.DMA((2,)),
            pltpu.SemaphoreType.DMA((2,)),
            pltpu.SemaphoreType.DMA((2,)),
        ],
        compiler_params=pltpu.CompilerParams(
            collective_id=0, has_side_effects=True, vmem_limit_bytes=24 << 20
        ),
        name="krum",
    )(
        winner,
        pltpu.with_memory_space_constraint(neighbours, pltpu.HBM),
        pltpu.with_memory_space_constraint(
            gradients.reshape(length // LANES, LANES), pltpu.HBM
        ),
    )
    scores, aggregate = pl.pallas_call(
        finish,
        out_shape=(
            jax.ShapeDtypeStruct((WORKERS,), f32),
            jax.ShapeDtypeStruct((ROWS, LANES), f32),
        ),
        in_specs=[pl.BlockSpec(memory_space=pltpu.VMEM)] * 2,
        out_specs=(pl.BlockSpec(memory_space=pltpu.VMEM), pl.BlockSpec(memory_space=pltpu.HBM)),
        scratch_shapes=[pltpu.SemaphoreType.DMA],
        compiler_params=pltpu.CompilerParams(vmem_limit_bytes=1 << 20),
        name="finish",
    )(scores, aggregate)
    return scores, aggregate.reshape(-1)


def solution(mesh):
    split = Mesh(mesh.devices.reshape(4, 2, 2, 8, 2), AXES)
    in_specs = (P(WORKER, MP), P(), P())
    out_specs = (P(), P(MP_WORKER))
    return jax.shard_map(body, mesh=split, in_specs=in_specs, out_specs=out_specs, check_vma=False)
```

```python
import functools

import jax
import jax.numpy as jnp
from jax import lax
from jax.experimental import pallas as pl
from jax.experimental.pallas import tpu as pltpu
from jax.sharding import Mesh
from jax.sharding import PartitionSpec as P

AXES = ("y", "xh", "c", "z", "xl")
WORKER = ("y", "xh", "c")
MP = ("z", "xl")
MP_WORKER = ("z", "xl", "y", "xh", "c")
MESH = pl.DeviceIdType.MESH

WORKERS = 16
ROWS = 256
LANES = 128

PAIR = (0, 0, 0, 1)
ACROSS = (2, 0, 0, 0)
PASSED = [(2, dy, 0, dc) for dy in (2, 1, 3) for dc in (0, 1)]
DIRECT = [(2, 0, 0, 1), ACROSS]
COLUMN = [(0, dy, 0, dc) for dy in (2, 1, 3) for dc in (0, 1)] + [PAIR]
CHIPS = [(2, 2), (2, 0), (0, 2), (2, 1), (0, 1), (2, 3), (0, 3)]
SIDES = [(1, 0, 0, 0), (3, 0, 0, 0)]
ENDS = [(0, 0, 1, 0), (0, 0, 7, 0)]
ROUNDS = 4
SLICE = [
    (dx, dy, dz, 0)
    for dx, dy, dz in sorted(
        ((a, b, d) for a in range(4) for b in range(4) for d in range(8)),
        key=lambda p: -(min(p[0], 4 - p[0]) + min(p[1], 4 - p[1]) + min(p[2], 8 - p[2])),
    )
    if (dx, dy, dz) != (0, 0, 0)
]


class Place:
    def __init__(self):
        x = lax.axis_index("xh") * 2 + lax.axis_index("xl")
        own = (x, lax.axis_index("y"), lax.axis_index("z"), lax.axis_index("c"))
        self.steps = [
            [value] + [lax.rem(value + step, size) for step in range(1, size)]
            for value, size in zip(own, (4, 4, 8, 2))
        ]
        self.x_hi = [x // 2 for x in self.steps[0]]
        self.x_lo = [lax.rem(x, 2) for x in self.steps[0]]

    def device(self, offset):
        dx, dy, dz, dc = offset
        _, y, z, c = self.steps
        return {"y": y[dy], "xh": self.x_hi[dx], "c": c[dc], "z": z[dz], "xl": self.x_lo[dx]}

    def chip(self, offset):
        return self.steps[1][offset[1]] * 2 + self.x_hi[offset[0]]

    def worker(self, offset):
        return self.chip(offset) * 2 + self.steps[3][offset[3]]

    def signal(self, sem, offset):
        pl.semaphore_signal(sem, inc=1, device_id=self.device(offset), device_id_type=MESH)

    def send(self, src, dst, send_sem, recv_sem, offset):
        pltpu.make_async_remote_copy(
            src_ref=src,
            dst_ref=dst,
            send_sem=send_sem,
            recv_sem=recv_sem,
            device_id=self.device(offset),
            device_id_type=MESH,
        ).start()


def wait_bytes(ref, sem):
    pltpu.make_async_copy(ref, ref, sem).wait()


def kernel(
    total_entries,
    winner_ref,
    neighbours_hbm,
    gradients_ref,
    scores_ref,
    aggregate_ref,
    full,
    hi,
    passing,
    got,
    lo,
    lo_away,
    lo_mine,
    lo_got,
    own_sum,
    pair_got,
    pair_sum,
    sums_got,
    neighbours_ref,
    load_sem,
    hi_send,
    hi_recv,
    pass_recv,
    lo_send,
    lo_recv,
    sum_send,
    sum_recv,
    plane_in,
    line_in,
):
    here = Place()
    home = (0, 0, 0, 0)
    own_core = here.steps[3][0]
    own_chip = here.chip(home)
    own = here.worker(home)

    order = PASSED + COLUMN + DIRECT + [home]
    loads = []
    for slot, offset in enumerate(order):
        rows = pl.ds(pl.multiple_of(here.worker(offset) * ROWS, ROWS), ROWS)
        load = pltpu.make_async_copy(gradients_ref.at[rows], full.at[slot], load_sem.at[slot])
        load.start()
        loads.append(load)
    fetch = pltpu.make_async_copy(neighbours_hbm, neighbours_ref, load_sem.at[WORKERS])
    fetch.start()

    barrier = pltpu.get_barrier_semaphore()
    partners = COLUMN + DIRECT + SIDES + ENDS
    for offset in partners:
        here.signal(barrier, offset)

    for slot, offset in enumerate(order):
        loads[slot].wait()
        value = full[slot]
        high = value.astype(jnp.bfloat16)
        low = (value - high.astype(jnp.float32)).astype(jnp.bfloat16)
        if offset == home:
            got[own] = high
        else:
            hi[slot] = high
        if offset[3] == 0:
            lo[own_core, here.chip(offset)] = low
        else:
            lo_away[here.chip(offset)] = low

    pl.semaphore_wait(barrier, len(partners))

    for slot, offset in enumerate(order):
        if offset in PASSED:
            here.send(hi.at[slot], passing.at[slot], hi_send, pass_recv.at[slot], ACROSS)
    for slot, offset in enumerate(order):
        if offset in COLUMN + DIRECT:
            here.send(hi.at[slot], got.at[own], hi_send, hi_recv, offset)
    for offset in SIDES + [ACROSS]:
        here.signal(plane_in, offset)
    here.send(lo_away, lo.at[own_core], lo_send.at[0], lo_recv.at[0], PAIR)

    fetch.wait()
    winner = winner_ref[0]
    row = lax.broadcasted_iota(jnp.int32, (WORKERS, ROWS), 0)
    column = lax.broadcasted_iota(jnp.int32, (WORKERS, ROWS), 1) // 16
    counts = jnp.zeros((WORKERS, ROWS), jnp.float32)
    for entry in range(neighbours_ref.shape[1]):
        counts += (neighbours_ref[:, entry : entry + 1] == column).astype(jnp.float32)
    own_sum[...] = jnp.zeros_like(own_sum)

    wait_bytes(lo_away, lo_recv.at[0])
    lo_mine[...] = lo[lax.rem(winner, 2)]

    pl.semaphore_wait(plane_in, len(SIDES) + 1)
    across = here.worker(ACROSS)
    for slot, (_, dy, _, dc) in enumerate(PASSED):
        if slot < ROUNDS:
            for offset in ENDS:
                here.signal(line_in.at[slot], offset)
        wait_bytes(passing.at[slot], pass_recv.at[slot])
        here.send(passing.at[slot], got.at[across], hi_send, hi_recv, (0, dy, 0, dc))
        if slot < ROUNDS:
            pl.semaphore_wait(line_in.at[slot], len(ENDS))

    wait_bytes(got.at[pl.ds(0, 15)], hi_recv)
    for dx, dy in CHIPS:
        offset = (dx, dy, 0, 0)
        here.send(
            lo_mine.at[here.chip(offset)],
            lo_got.at[own_chip],
            lo_send.at[1],
            lo_recv.at[1],
            offset,
        )
    lo_got[own_chip] = lo_mine[own_chip]

    parts = [got[:, pl.ds(step * 16, 16), :].reshape(ROWS, LANES) for step in range(ROWS // 16)]
    block = jnp.concatenate(parts, axis=1)
    total = lax.dot_general(
        block, block, (((1,), (1,)), ((), ())), preferred_element_type=jnp.float32
    )
    sublane = lax.broadcasted_iota(jnp.int32, (ROWS, ROWS), 0)
    lane = lax.broadcasted_iota(jnp.int32, (ROWS, ROWS), 1)
    total = jnp.where(lax.rem(sublane, 16) == lax.rem(lane, 16), total, 0.0)
    total = jnp.sum(total.reshape(WORKERS, 16, ROWS), axis=1)
    diagonal = jnp.where(row == column, total, 0.0)
    squares = jnp.sum(diagonal, axis=0, keepdims=True)
    own_counts = jnp.sum(counts, axis=1, keepdims=True) * (1.0 / 16.0)
    partial = counts * (squares - 2.0 * total) + own_counts * diagonal
    partial = lax.dot_general(
        jnp.ones((8, ROWS), jnp.float32),
        partial,
        (((1,), (1,)), ((), ())),
        precision=lax.Precision.HIGHEST,
        preferred_element_type=jnp.float32,
    )
    own_sum[:, pl.ds(0, WORKERS)] = partial[0:1]

    here.send(own_sum, pair_got, sum_send.at[0], sum_recv.at[0], PAIR)
    wait_bytes(pair_got, sum_recv.at[0])
    pair_sum[...] = own_sum[...] + pair_got[...]
    for step, offset in enumerate(SLICE):
        here.send(pair_sum, sums_got.at[step], sum_send.at[1], sum_recv.at[1], offset)

    wait_bytes(lo_got.at[pl.ds(0, 7)], lo_recv.at[1])
    aggregate_ref[...] = got[winner].astype(jnp.float32) + lo_got[winner // 2].astype(jnp.float32)

    wait_bytes(sums_got, sum_recv.at[1])
    scores = pair_sum[...] + jnp.sum(sums_got[...], axis=0)
    scores_ref[...] = scores / jnp.float32(total_entries)

    wait_bytes(got.at[pl.ds(0, 15)], hi_send)
    wait_bytes(passing, hi_send)
    wait_bytes(lo_away, lo_send.at[0])
    wait_bytes(lo_got.at[pl.ds(0, 7)], lo_send.at[1])
    wait_bytes(pair_got, sum_send.at[0])
    wait_bytes(sums_got, sum_send.at[1])


def finish(row_ref, block_ref, scores_ref, aggregate_ref, sem):
    copy = pltpu.make_async_copy(block_ref, aggregate_ref, sem)
    copy.start()
    scores_ref[...] = row_ref[0, :WORKERS]
    copy.wait()


def body(gradients, neighbours, winner):
    length = gradients.shape[1]
    total_entries = neighbours.shape[1] * length * lax.axis_size(MP)
    bf16, f32 = jnp.bfloat16, jnp.float32
    out_shape = (
        jax.ShapeDtypeStruct((1, LANES), f32),
        jax.ShapeDtypeStruct((ROWS, LANES), f32),
    )
    scores, aggregate = pl.pallas_call(
        functools.partial(kernel, total_entries),
        out_shape=out_shape,
        in_specs=[
            pl.BlockSpec(memory_space=pltpu.SMEM),
            pl.BlockSpec(memory_space=pltpu.HBM),
            pl.BlockSpec(memory_space=pltpu.HBM),
        ],
        out_specs=(pl.BlockSpec(memory_space=pltpu.VMEM),) * 2,
        scratch_shapes=[
            pltpu.VMEM((WORKERS, ROWS, LANES), f32),
            pltpu.VMEM((15, ROWS, LANES), bf16),
            pltpu.VMEM((len(PASSED), ROWS, LANES), bf16),
            pltpu.VMEM((WORKERS, ROWS, LANES), bf16),
            pltpu.VMEM((2, 8, ROWS, LANES), bf16),
            pltpu.VMEM((8, ROWS, LANES), bf16),
            pltpu.VMEM((8, ROWS, LANES), bf16),
            pltpu.VMEM((8, ROWS, LANES), bf16),
            pltpu.VMEM((1, LANES), f32),
            pltpu.VMEM((1, LANES), f32),
            pltpu.VMEM((1, LANES), f32),
            pltpu.VMEM((len(SLICE), 1, LANES), f32),
            pltpu.VMEM(neighbours.shape, jnp.int32),
            pltpu.SemaphoreType.DMA((WORKERS + 1,)),
            pltpu.SemaphoreType.DMA,
            pltpu.SemaphoreType.DMA,
            pltpu.SemaphoreType.DMA((len(PASSED),)),
            pltpu.SemaphoreType.DMA((2,)),
            pltpu.SemaphoreType.DMA((2,)),
            pltpu.SemaphoreType.DMA((2,)),
            pltpu.SemaphoreType.DMA((2,)),
            pltpu.SemaphoreType.REGULAR,
            pltpu.SemaphoreType.REGULAR((ROUNDS,)),
        ],
        compiler_params=pltpu.CompilerParams(
            collective_id=0, has_side_effects=True, vmem_limit_bytes=24 << 20
        ),
        name="krum",
    )(
        winner,
        pltpu.with_memory_space_constraint(neighbours, pltpu.HBM),
        pltpu.with_memory_space_constraint(
            gradients.reshape(length // LANES, LANES), pltpu.HBM
        ),
    )
    scores, aggregate = pl.pallas_call(
        finish,
        out_shape=(jax.ShapeDtypeStruct((WORKERS,), f32), out_shape[1]),
        in_specs=[pl.BlockSpec(memory_space=pltpu.VMEM)] * 2,
        out_specs=(pl.BlockSpec(memory_space=pltpu.VMEM), pl.BlockSpec(memory_space=pltpu.HBM)),
        scratch_shapes=[pltpu.SemaphoreType.DMA],
        compiler_params=pltpu.CompilerParams(vmem_limit_bytes=1 << 20),
        name="finish",
    )(scores, aggregate)
    return scores, aggregate.reshape(-1)


def solution(mesh):
    split = Mesh(mesh.devices.reshape(4, 2, 2, 8, 2), AXES)
    in_specs = (P(WORKER, MP), P(), P())
    out_specs = (P(), P(MP_WORKER))
    return jax.shard_map(body, mesh=split, in_specs=in_specs, out_specs=out_specs, check_vma=False)
```

```python
import functools

import jax
import jax.numpy as jnp
from jax import lax
from jax.experimental import pallas as pl
from jax.experimental.pallas import tpu as pltpu
from jax.sharding import Mesh
from jax.sharding import PartitionSpec as P

AXES = ("y", "xh", "c", "z", "xl")
WORKER = ("y", "xh", "c")
MP = ("z", "xl")
MP_WORKER = ("z", "xl", "y", "xh", "c")
MESH = pl.DeviceIdType.MESH

WORKERS = 16
ROWS = 256
LANES = 128

PAIR = (0, 0, 0, 1)
ACROSS = (2, 0, 0, 0)
PASSED = [(2, dy, 0, dc) for dy, dc in ((2, 0), (2, 1), (1, 0), (3, 0), (1, 1), (3, 1))]
DIRECT = [(2, 0, 0, 1), ACROSS]
COLUMN = [(0, dy, 0, dc) for dy in (2, 1, 3) for dc in (0, 1)] + [PAIR]
LOW_ACROSS = [(2, dy, 0, 0) for dy in (2, 1, 3, 0)]
LOW_COLUMN = [(0, dy, 0, 0) for dy in (2, 1, 3)]
SIDES = [(1, 0, 0, 0), (3, 0, 0, 0)]
ENDS = [(0, 0, 1, 0), (0, 0, 7, 0)]
ROUNDS = 4
SLICE = [
    (dx, dy, dz, 0)
    for dx, dy, dz in sorted(
        ((a, b, d) for a in range(4) for b in range(4) for d in range(8)),
        key=lambda p: -(min(p[0], 4 - p[0]) + min(p[1], 4 - p[1]) + min(p[2], 8 - p[2])),
    )
    if (dx, dy, dz) != (0, 0, 0)
]


class Place:
    def __init__(self):
        x = lax.axis_index("xh") * 2 + lax.axis_index("xl")
        own = (x, lax.axis_index("y"), lax.axis_index("z"), lax.axis_index("c"))
        self.steps = [
            [value] + [lax.rem(value + step, size) for step in range(1, size)]
            for value, size in zip(own, (4, 4, 8, 2))
        ]
        self.x_hi = [x // 2 for x in self.steps[0]]
        self.x_lo = [lax.rem(x, 2) for x in self.steps[0]]

    def device(self, offset):
        dx, dy, dz, dc = offset
        _, y, z, c = self.steps
        return {"y": y[dy], "xh": self.x_hi[dx], "c": c[dc], "z": z[dz], "xl": self.x_lo[dx]}

    def chip(self, offset):
        return self.steps[1][offset[1]] * 2 + self.x_hi[offset[0]]

    def worker(self, offset):
        return self.chip(offset) * 2 + self.steps[3][offset[3]]

    def signal(self, sem, offset):
        pl.semaphore_signal(sem, inc=1, device_id=self.device(offset), device_id_type=MESH)

    def send(self, src, dst, send_sem, recv_sem, offset):
        pltpu.make_async_remote_copy(
            src_ref=src,
            dst_ref=dst,
            send_sem=send_sem,
            recv_sem=recv_sem,
            device_id=self.device(offset),
            device_id_type=MESH,
        ).start()


def wait_bytes(ref, sem):
    pltpu.make_async_copy(ref, ref, sem).wait()


def kernel(
    total_entries,
    winner_ref,
    neighbours_hbm,
    gradients_ref,
    scores_ref,
    aggregate_ref,
    full,
    hi,
    passing,
    got,
    lo,
    lo_away,
    lo_mine,
    lo_got,
    own_sum,
    pair_got,
    pair_sum,
    sums_got,
    neighbours_ref,
    load_sem,
    hi_send,
    hi_recv,
    pass_recv,
    lo_send,
    lo_recv,
    sum_send,
    sum_recv,
    plane_in,
    line_in,
):
    here = Place()
    home = (0, 0, 0, 0)
    own_core = here.steps[3][0]
    own_chip = here.chip(home)
    own = here.worker(home)

    order = PASSED + COLUMN + DIRECT + [home]
    loads = []
    for slot, offset in enumerate(order):
        rows = pl.ds(pl.multiple_of(here.worker(offset) * ROWS, ROWS), ROWS)
        load = pltpu.make_async_copy(gradients_ref.at[rows], full.at[slot], load_sem.at[slot])
        load.start()
        loads.append(load)
    fetch = pltpu.make_async_copy(neighbours_hbm, neighbours_ref, load_sem.at[WORKERS])
    fetch.start()

    barrier = pltpu.get_barrier_semaphore()
    partners = COLUMN + DIRECT + SIDES + ENDS
    for offset in partners:
        here.signal(barrier, offset)

    def start(slot):
        offset = order[slot]
        if offset in PASSED:
            here.send(hi.at[slot], passing.at[slot], hi_send, pass_recv.at[slot], ACROSS)
        elif offset != home:
            here.send(hi.at[slot], got.at[own], hi_send, hi_recv, offset)

    for slot, offset in enumerate(order):
        loads[slot].wait()
        value = full[slot]
        high = value.astype(jnp.bfloat16)
        low = (value - high.astype(jnp.float32)).astype(jnp.bfloat16)
        if offset == home:
            got[own] = high
        else:
            hi[slot] = high
        if offset[3] == 0:
            lo[own_core, here.chip(offset)] = low
        else:
            lo_away[here.chip(offset)] = low
        if slot == 1:
            pl.semaphore_wait(barrier, len(partners))
            for ready in range(1 + 1):
                start(ready)
        if slot > 1:
            start(slot)

    for offset in SIDES + [ACROSS]:
        here.signal(plane_in, offset)
    here.send(lo_away, lo.at[own_core], lo_send.at[0], lo_recv.at[0], PAIR)

    fetch.wait()
    winner = winner_ref[0]
    row = lax.broadcasted_iota(jnp.int32, (WORKERS, ROWS), 0)
    column = lax.broadcasted_iota(jnp.int32, (WORKERS, ROWS), 1) // 16
    counts = jnp.zeros((WORKERS, ROWS), jnp.float32)
    for entry in range(neighbours_ref.shape[1]):
        counts += (neighbours_ref[:, entry : entry + 1] == column).astype(jnp.float32)
    own_sum[...] = jnp.zeros_like(own_sum)

    wait_bytes(lo_away, lo_recv.at[0])
    lo_mine[...] = lo[lax.rem(winner, 2)]

    pl.semaphore_wait(plane_in, len(SIDES) + 1)
    across = here.worker(ACROSS)
    for slot, (_, dy, _, dc) in enumerate(PASSED):
        if slot < ROUNDS:
            for offset in ENDS:
                here.signal(line_in.at[slot], offset)
        wait_bytes(passing.at[slot], pass_recv.at[slot])
        here.send(passing.at[slot], got.at[across], hi_send, hi_recv, (0, dy, 0, dc))
        if slot < ROUNDS:
            pl.semaphore_wait(line_in.at[slot], len(ENDS))

    wait_bytes(got.at[pl.ds(0, 15)], hi_recv)
    lo_got[own_chip] = lo_mine[own_chip]

    for offset in LOW_ACROSS + LOW_COLUMN:
        here.send(
            lo_mine.at[here.chip(offset)],
            lo_got.at[own_chip],
            lo_send.at[1],
            lo_recv.at[1],
            offset,
        )
    parts = [got[:, pl.ds(step * 16, 16), :].reshape(ROWS, LANES) for step in range(ROWS // 16)]
    block = jnp.concatenate(parts, axis=1)
    total = lax.dot_general(
        block, block, (((1,), (1,)), ((), ())), preferred_element_type=jnp.float32
    )
    sublane = lax.broadcasted_iota(jnp.int32, (ROWS, ROWS), 0)
    lane = lax.broadcasted_iota(jnp.int32, (ROWS, ROWS), 1)
    total = jnp.where(lax.rem(sublane, 16) == lax.rem(lane, 16), total, 0.0)
    total = jnp.sum(total.reshape(WORKERS, 16, ROWS), axis=1)
    diagonal = jnp.where(row == column, total, 0.0)
    squares = jnp.sum(diagonal, axis=0, keepdims=True)
    own_counts = jnp.sum(counts, axis=1, keepdims=True) * (1.0 / 16.0)
    partial = counts * (squares - 2.0 * total) + own_counts * diagonal
    partial = lax.dot_general(
        jnp.ones((8, ROWS), jnp.float32),
        partial,
        (((1,), (1,)), ((), ())),
        precision=lax.Precision.HIGHEST,
        preferred_element_type=jnp.float32,
    )
    own_sum[:, pl.ds(0, WORKERS)] = partial[0:1]

    here.send(own_sum, pair_got, sum_send.at[0], sum_recv.at[0], PAIR)
    wait_bytes(pair_got, sum_recv.at[0])
    pair_sum[...] = own_sum[...] + pair_got[...]
    for step, offset in enumerate(SLICE):
        here.send(pair_sum, sums_got.at[step], sum_send.at[1], sum_recv.at[1], offset)

    wait_bytes(lo_got.at[pl.ds(0, 7)], lo_recv.at[1])
    aggregate_ref[...] = got[winner].astype(jnp.float32) + lo_got[winner // 2].astype(jnp.float32)

    wait_bytes(sums_got, sum_recv.at[1])
    scores = pair_sum[...] + jnp.sum(sums_got[...], axis=0)
    scores_ref[...] = scores / jnp.float32(total_entries)

    wait_bytes(got.at[pl.ds(0, 15)], hi_send)
    wait_bytes(passing, hi_send)
    wait_bytes(lo_away, lo_send.at[0])
    wait_bytes(lo_got.at[pl.ds(0, 7)], lo_send.at[1])
    wait_bytes(pair_got, sum_send.at[0])
    wait_bytes(sums_got, sum_send.at[1])


def finish(row_ref, block_ref, scores_ref, aggregate_ref, sem):
    copy = pltpu.make_async_copy(block_ref, aggregate_ref, sem)
    copy.start()
    scores_ref[...] = row_ref[0, :WORKERS]
    copy.wait()


def body(gradients, neighbours, winner):
    length = gradients.shape[1]
    total_entries = neighbours.shape[1] * length * lax.axis_size(MP)
    bf16, f32 = jnp.bfloat16, jnp.float32
    out_shape = (
        jax.ShapeDtypeStruct((1, LANES), f32),
        jax.ShapeDtypeStruct((ROWS, LANES), f32),
    )
    scores, aggregate = pl.pallas_call(
        functools.partial(kernel, total_entries),
        out_shape=out_shape,
        in_specs=[
            pl.BlockSpec(memory_space=pltpu.SMEM),
            pl.BlockSpec(memory_space=pltpu.HBM),
            pl.BlockSpec(memory_space=pltpu.HBM),
        ],
        out_specs=(pl.BlockSpec(memory_space=pltpu.VMEM),) * 2,
        scratch_shapes=[
            pltpu.VMEM((WORKERS, ROWS, LANES), f32),
            pltpu.VMEM((15, ROWS, LANES), bf16),
            pltpu.VMEM((len(PASSED), ROWS, LANES), bf16),
            pltpu.VMEM((WORKERS, ROWS, LANES), bf16),
            pltpu.VMEM((2, 8, ROWS, LANES), bf16),
            pltpu.VMEM((8, ROWS, LANES), bf16),
            pltpu.VMEM((8, ROWS, LANES), bf16),
            pltpu.VMEM((8, ROWS, LANES), bf16),
            pltpu.VMEM((1, LANES), f32),
            pltpu.VMEM((1, LANES), f32),
            pltpu.VMEM((1, LANES), f32),
            pltpu.VMEM((len(SLICE), 1, LANES), f32),
            pltpu.VMEM(neighbours.shape, jnp.int32),
            pltpu.SemaphoreType.DMA((WORKERS + 1,)),
            pltpu.SemaphoreType.DMA,
            pltpu.SemaphoreType.DMA,
            pltpu.SemaphoreType.DMA((len(PASSED),)),
            pltpu.SemaphoreType.DMA((2,)),
            pltpu.SemaphoreType.DMA((2,)),
            pltpu.SemaphoreType.DMA((2,)),
            pltpu.SemaphoreType.DMA((2,)),
            pltpu.SemaphoreType.REGULAR,
            pltpu.SemaphoreType.REGULAR((ROUNDS,)),
        ],
        compiler_params=pltpu.CompilerParams(
            collective_id=0, has_side_effects=True, vmem_limit_bytes=24 << 20
        ),
        name="krum",
    )(
        winner,
        pltpu.with_memory_space_constraint(neighbours, pltpu.HBM),
        pltpu.with_memory_space_constraint(
            gradients.reshape(length // LANES, LANES), pltpu.HBM
        ),
    )
    scores, aggregate = pl.pallas_call(
        finish,
        out_shape=(jax.ShapeDtypeStruct((WORKERS,), f32), out_shape[1]),
        in_specs=[pl.BlockSpec(memory_space=pltpu.VMEM)] * 2,
        out_specs=(pl.BlockSpec(memory_space=pltpu.VMEM), pl.BlockSpec(memory_space=pltpu.HBM)),
        scratch_shapes=[pltpu.SemaphoreType.DMA],
        compiler_params=pltpu.CompilerParams(vmem_limit_bytes=1 << 20),
        name="finish",
    )(scores, aggregate)
    return scores, aggregate.reshape(-1)


def solution(mesh):
    split = Mesh(mesh.devices.reshape(4, 2, 2, 8, 2), AXES)
    in_specs = (P(WORKER, MP), P(), P())
    out_specs = (P(), P(MP_WORKER))
    return jax.shard_map(body, mesh=split, in_specs=in_specs, out_specs=out_specs, check_vma=False)
```

```python
import functools

import jax
import jax.numpy as jnp
from jax import lax
from jax.experimental import pallas as pl
from jax.experimental.pallas import tpu as pltpu
from jax.sharding import Mesh
from jax.sharding import PartitionSpec as P

AXES = ("y", "xh", "c", "z", "xl")
WORKER = ("y", "xh", "c")
MP = ("z", "xl")
MP_WORKER = ("z", "xl", "y", "xh", "c")
MESH = pl.DeviceIdType.MESH

WORKERS = 16
ROWS = 256
LANES = 128

PAIR = (0, 0, 0, 1)
ACROSS = (2, 0, 0, 0)
PASSED = [(2, dy, 0, dc) for dy, dc in ((2, 0), (2, 1),)]
LATE = [(2, dy, 0, dc) for dy, dc in ((1, 0), (3, 0), (1, 1), (3, 1),)]
DIRECT = [(2, 0, 0, 1), ACROSS]
COLUMN = [(0, dy, 0, dc) for dy in (2, 1, 3) for dc in (0, 1)] + [PAIR]
LOW_ACROSS = [(2, dy, 0, 0) for dy in (2, 1, 3, 0)]
LOW_COLUMN = [(0, dy, 0, 0) for dy in (2, 1, 3)]
SIDES = [(1, 0, 0, 0), (3, 0, 0, 0)]
ENDS = [(0, 0, 1, 0), (0, 0, 7, 0)]
ROUNDS = 4
SLICE = [
    (dx, dy, dz, 0)
    for dx, dy, dz in sorted(
        ((a, b, d) for a in range(4) for b in range(4) for d in range(8)),
        key=lambda p: -(min(p[0], 4 - p[0]) + min(p[1], 4 - p[1]) + min(p[2], 8 - p[2])),
    )
    if (dx, dy, dz) != (0, 0, 0)
]


class Place:
    def __init__(self):
        x = lax.axis_index("xh") * 2 + lax.axis_index("xl")
        own = (x, lax.axis_index("y"), lax.axis_index("z"), lax.axis_index("c"))
        self.steps = [
            [value] + [lax.rem(value + step, size) for step in range(1, size)]
            for value, size in zip(own, (4, 4, 8, 2))
        ]
        self.x_hi = [x // 2 for x in self.steps[0]]
        self.x_lo = [lax.rem(x, 2) for x in self.steps[0]]

    def device(self, offset):
        dx, dy, dz, dc = offset
        _, y, z, c = self.steps
        return {"y": y[dy], "xh": self.x_hi[dx], "c": c[dc], "z": z[dz], "xl": self.x_lo[dx]}

    def chip(self, offset):
        return self.steps[1][offset[1]] * 2 + self.x_hi[offset[0]]

    def worker(self, offset):
        return self.chip(offset) * 2 + self.steps[3][offset[3]]

    def signal(self, sem, offset):
        pl.semaphore_signal(sem, inc=1, device_id=self.device(offset), device_id_type=MESH)

    def send(self, src, dst, send_sem, recv_sem, offset):
        pltpu.make_async_remote_copy(
            src_ref=src,
            dst_ref=dst,
            send_sem=send_sem,
            recv_sem=recv_sem,
            device_id=self.device(offset),
            device_id_type=MESH,
        ).start()


def wait_bytes(ref, sem):
    pltpu.make_async_copy(ref, ref, sem).wait()


def kernel(
    total_entries,
    winner_ref,
    neighbours_hbm,
    gradients_ref,
    scores_ref,
    aggregate_ref,
    full,
    hi,
    passing,
    got,
    lo,
    lo_away,
    lo_mine,
    lo_got,
    own_sum,
    pair_got,
    pair_sum,
    sums_got,
    neighbours_ref,
    load_sem,
    hi_send,
    hi_recv,
    pass_recv,
    lo_send,
    lo_recv,
    sum_send,
    sum_recv,
    plane_in,
    line_in,
):
    here = Place()
    home = (0, 0, 0, 0)
    own_core = here.steps[3][0]
    own_chip = here.chip(home)
    own = here.worker(home)

    barrier = pltpu.get_barrier_semaphore()
    partners = COLUMN + DIRECT + SIDES + ENDS
    for offset in partners:
        here.signal(barrier, offset)

    order = PASSED + COLUMN + DIRECT + LATE + [home]
    loads = []
    for slot, offset in enumerate(order):
        rows = pl.ds(pl.multiple_of(here.worker(offset) * ROWS, ROWS), ROWS)
        load = pltpu.make_async_copy(gradients_ref.at[rows], full.at[slot], load_sem.at[slot])
        load.start()
        loads.append(load)
    fetch = pltpu.make_async_copy(neighbours_hbm, neighbours_ref, load_sem.at[WORKERS])
    fetch.start()

    def start(slot):
        offset = order[slot]
        if offset in PASSED:
            here.send(hi.at[slot], passing.at[slot], hi_send, pass_recv.at[slot], ACROSS)
        elif offset != home and offset not in LATE:
            here.send(hi.at[slot], got.at[own], hi_send, hi_recv, offset)

    for slot, offset in enumerate(order):
        loads[slot].wait()
        value = full[slot]
        high = value.astype(jnp.bfloat16)
        low = (value - high.astype(jnp.float32)).astype(jnp.bfloat16)
        if offset == home:
            got[own] = high
        else:
            hi[slot] = high
        if offset[3] == 0:
            lo[own_core, here.chip(offset)] = low
        else:
            lo_away[here.chip(offset)] = low
        if slot == 1:
            pl.semaphore_wait(barrier, len(partners))
            for ready in range(1 + 1):
                start(ready)
        if slot > 1:
            start(slot)

    for offset in SIDES + [ACROSS]:
        here.signal(plane_in, offset)
    here.send(lo_away, lo.at[own_core], lo_send.at[0], lo_recv.at[0], PAIR)

    fetch.wait()
    winner = winner_ref[0]
    row = lax.broadcasted_iota(jnp.int32, (WORKERS, ROWS), 0)
    column = lax.broadcasted_iota(jnp.int32, (WORKERS, ROWS), 1) // 16
    counts = jnp.zeros((WORKERS, ROWS), jnp.float32)
    for entry in range(neighbours_ref.shape[1]):
        counts += (neighbours_ref[:, entry : entry + 1] == column).astype(jnp.float32)
    own_sum[...] = jnp.zeros_like(own_sum)

    wait_bytes(lo_away, lo_recv.at[0])
    lo_mine[...] = lo[lax.rem(winner, 2)]

    pl.semaphore_wait(plane_in, len(SIDES) + 1)
    for slot, offset in enumerate(order):
        if offset in LATE:
            here.send(hi.at[slot], got.at[own], hi_send, hi_recv, offset)
    across = here.worker(ACROSS)
    for slot in range(max(ROUNDS, len(PASSED))):
        if slot < ROUNDS:
            for offset in ENDS:
                here.signal(line_in.at[slot], offset)
        if slot < len(PASSED):
            _, dy, _, dc = PASSED[slot]
            wait_bytes(passing.at[slot], pass_recv.at[slot])
            here.send(passing.at[slot], got.at[across], hi_send, hi_recv, (0, dy, 0, dc))
        if slot < ROUNDS:
            pl.semaphore_wait(line_in.at[slot], len(ENDS))

    wait_bytes(got.at[pl.ds(0, 15)], hi_recv)
    lo_got[own_chip] = lo_mine[own_chip]

    for offset in LOW_ACROSS + LOW_COLUMN:
        here.send(
            lo_mine.at[here.chip(offset)],
            lo_got.at[own_chip],
            lo_send.at[1],
            lo_recv.at[1],
            offset,
        )
    parts = [got[:, pl.ds(step * 16, 16), :].reshape(ROWS, LANES) for step in range(ROWS // 16)]
    block = jnp.concatenate(parts, axis=1)
    total = lax.dot_general(
        block, block, (((1,), (1,)), ((), ())), preferred_element_type=jnp.float32
    )
    sublane = lax.broadcasted_iota(jnp.int32, (ROWS, ROWS), 0)
    lane = lax.broadcasted_iota(jnp.int32, (ROWS, ROWS), 1)
    total = jnp.where(lax.rem(sublane, 16) == lax.rem(lane, 16), total, 0.0)
    total = jnp.sum(total.reshape(WORKERS, 16, ROWS), axis=1)
    diagonal = jnp.where(row == column, total, 0.0)
    squares = jnp.sum(diagonal, axis=0, keepdims=True)
    own_counts = jnp.sum(counts, axis=1, keepdims=True) * (1.0 / 16.0)
    partial = counts * (squares - 2.0 * total) + own_counts * diagonal
    partial = lax.dot_general(
        jnp.ones((8, ROWS), jnp.float32),
        partial,
        (((1,), (1,)), ((), ())),
        precision=lax.Precision.HIGHEST,
        preferred_element_type=jnp.float32,
    )
    own_sum[:, pl.ds(0, WORKERS)] = partial[0:1]

    here.send(own_sum, pair_got, sum_send.at[0], sum_recv.at[0], PAIR)
    wait_bytes(pair_got, sum_recv.at[0])
    pair_sum[...] = own_sum[...] + pair_got[...]
    for step, offset in enumerate(SLICE):
        here.send(pair_sum, sums_got.at[step], sum_send.at[1], sum_recv.at[1], offset)

    wait_bytes(lo_got.at[pl.ds(0, 7)], lo_recv.at[1])
    aggregate_ref[...] = got[winner].astype(jnp.float32) + lo_got[winner // 2].astype(jnp.float32)

    wait_bytes(sums_got, sum_recv.at[1])
    scores = pair_sum[...] + jnp.sum(sums_got[...], axis=0)
    scores_ref[...] = scores[0, :WORKERS] / jnp.float32(total_entries)

    wait_bytes(got.at[pl.ds(0, 15)], hi_send)
    wait_bytes(passing, hi_send)
    wait_bytes(lo_away, lo_send.at[0])
    wait_bytes(lo_got.at[pl.ds(0, 7)], lo_send.at[1])
    wait_bytes(pair_got, sum_send.at[0])
    wait_bytes(sums_got, sum_send.at[1])


def finish(scores_ref, block_ref, scores_hbm, block_hbm, sem):
    copies = (
        pltpu.make_async_copy(scores_ref, scores_hbm, sem.at[0]),
        pltpu.make_async_copy(block_ref, block_hbm, sem.at[1]),
    )
    for copy in copies:
        copy.start()
    for copy in copies:
        copy.wait()


def body(gradients, neighbours, winner):
    length = gradients.shape[1]
    total_entries = neighbours.shape[1] * length * lax.axis_size(MP)
    bf16, f32 = jnp.bfloat16, jnp.float32
    out_shape = (
        jax.ShapeDtypeStruct((WORKERS,), f32),
        jax.ShapeDtypeStruct((ROWS, LANES), f32),
    )
    scores, aggregate = pl.pallas_call(
        functools.partial(kernel, total_entries),
        out_shape=out_shape,
        in_specs=[
            pl.BlockSpec(memory_space=pltpu.SMEM),
            pl.BlockSpec(memory_space=pltpu.HBM),
            pl.BlockSpec(memory_space=pltpu.HBM),
        ],
        out_specs=(pl.BlockSpec(memory_space=pltpu.VMEM),) * 2,
        scratch_shapes=[
            pltpu.VMEM((WORKERS, ROWS, LANES), f32),
            pltpu.VMEM((15, ROWS, LANES), bf16),
            pltpu.VMEM((len(PASSED), ROWS, LANES), bf16),
            pltpu.VMEM((WORKERS, ROWS, LANES), bf16),
            pltpu.VMEM((2, 8, ROWS, LANES), bf16),
            pltpu.VMEM((8, ROWS, LANES), bf16),
            pltpu.VMEM((8, ROWS, LANES), bf16),
            pltpu.VMEM((8, ROWS, LANES), bf16),
            pltpu.VMEM((1, LANES), f32),
            pltpu.VMEM((1, LANES), f32),
            pltpu.VMEM((1, LANES), f32),
            pltpu.VMEM((len(SLICE), 1, LANES), f32),
            pltpu.VMEM(neighbours.shape, jnp.int32),
            pltpu.SemaphoreType.DMA((WORKERS + 1,)),
            pltpu.SemaphoreType.DMA,
            pltpu.SemaphoreType.DMA,
            pltpu.SemaphoreType.DMA((len(PASSED),)),
            pltpu.SemaphoreType.DMA((2,)),
            pltpu.SemaphoreType.DMA((2,)),
            pltpu.SemaphoreType.DMA((2,)),
            pltpu.SemaphoreType.DMA((2,)),
            pltpu.SemaphoreType.REGULAR,
            pltpu.SemaphoreType.REGULAR((ROUNDS,)),
        ],
        compiler_params=pltpu.CompilerParams(
            collective_id=0, has_side_effects=True, vmem_limit_bytes=24 << 20
        ),
        name="krum",
    )(
        winner,
        pltpu.with_memory_space_constraint(neighbours, pltpu.HBM),
        pltpu.with_memory_space_constraint(
            gradients.reshape(length // LANES, LANES), pltpu.HBM
        ),
    )
    scores, aggregate = pl.pallas_call(
        finish,
        out_shape=out_shape,
        in_specs=[pl.BlockSpec(memory_space=pltpu.VMEM)] * 2,
        out_specs=(pl.BlockSpec(memory_space=pltpu.HBM),) * 2,
        scratch_shapes=[pltpu.SemaphoreType.DMA((2,))],
        compiler_params=pltpu.CompilerParams(vmem_limit_bytes=1 << 20),
        name="finish",
    )(scores, aggregate)
    return scores, aggregate.reshape(-1)


def solution(mesh):
    split = Mesh(mesh.devices.reshape(4, 2, 2, 8, 2), AXES)
    in_specs = (P(WORKER, MP), P(), P())
    out_specs = (P(), P(MP_WORKER))
    return jax.shard_map(body, mesh=split, in_specs=in_specs, out_specs=out_specs, check_vma=False)
```

```python
import functools

import jax
import jax.numpy as jnp
from jax import lax
from jax.experimental import pallas as pl
from jax.experimental.pallas import tpu as pltpu
from jax.sharding import Mesh
from jax.sharding import PartitionSpec as P

AXES = ("y", "xh", "c", "z", "xl")
WORKER = ("y", "xh", "c")
MP = ("z", "xl")
MP_WORKER = ("z", "xl", "y", "xh", "c")
MESH = pl.DeviceIdType.MESH

WORKERS = 16
ROWS = 256
LANES = 128

PAIR = (0, 0, 0, 1)
ACROSS = (2, 0, 0, 0)
PASSED = [(2, dy, 0, dc) for dy, dc in ((2, 0), (2, 1),)]
LATE = [(2, dy, 0, dc) for dy, dc in ((1, 0), (3, 0), (1, 1), (3, 1),)]
DIRECT = [(2, 0, 0, 1), ACROSS]
COLUMN = [(0, dy, 0, dc) for dy in (2, 1, 3) for dc in (0, 1)] + [PAIR]
LOW_ACROSS = [(2, dy, 0, 0) for dy in (2, 1, 3, 0)]
LOW_COLUMN = [(0, dy, 0, 0) for dy in (2, 1, 3)]
SIDES = [(1, 0, 0, 0), (3, 0, 0, 0)]
ENDS = [(0, 0, 1, 0), (0, 0, 7, 0)]
ROUNDS = 4
SLICE = [
    (dx, dy, dz, 0)
    for dx, dy, dz in sorted(
        ((a, b, d) for a in range(4) for b in range(4) for d in range(8)),
        key=lambda p: -(min(p[0], 4 - p[0]) + min(p[1], 4 - p[1]) + min(p[2], 8 - p[2])),
    )
    if (dx, dy, dz) != (0, 0, 0)
]


class Place:
    def __init__(self):
        x = lax.axis_index("xh") * 2 + lax.axis_index("xl")
        own = (x, lax.axis_index("y"), lax.axis_index("z"), lax.axis_index("c"))
        self.steps = [
            [value] + [lax.rem(value + step, size) for step in range(1, size)]
            for value, size in zip(own, (4, 4, 8, 2))
        ]
        self.x_hi = [x // 2 for x in self.steps[0]]
        self.x_lo = [lax.rem(x, 2) for x in self.steps[0]]

    def device(self, offset):
        dx, dy, dz, dc = offset
        _, y, z, c = self.steps
        return {"y": y[dy], "xh": self.x_hi[dx], "c": c[dc], "z": z[dz], "xl": self.x_lo[dx]}

    def chip(self, offset):
        return self.steps[1][offset[1]] * 2 + self.x_hi[offset[0]]

    def worker(self, offset):
        return self.chip(offset) * 2 + self.steps[3][offset[3]]

    def signal(self, sem, offset):
        pl.semaphore_signal(sem, inc=1, device_id=self.device(offset), device_id_type=MESH)

    def send(self, src, dst, send_sem, recv_sem, offset):
        pltpu.make_async_remote_copy(
            src_ref=src,
            dst_ref=dst,
            send_sem=send_sem,
            recv_sem=recv_sem,
            device_id=self.device(offset),
            device_id_type=MESH,
        ).start()


def wait_bytes(ref, sem):
    pltpu.make_async_copy(ref, ref, sem).wait()


def kernel(
    total_entries,
    winner_ref,
    neighbours_hbm,
    gradients_ref,
    scores_ref,
    aggregate_ref,
    full,
    hi,
    passing,
    got,
    lo,
    lo_away,
    lo_mine,
    lo_got,
    own_sum,
    pair_got,
    pair_sum,
    sums_got,
    neighbours_ref,
    load_sem,
    hi_send,
    over_send,
    hi_recv,
    pass_recv,
    lo_send,
    lo_recv,
    sum_send,
    sum_recv,
    plane_in,
    line_in,
):
    here = Place()
    home = (0, 0, 0, 0)
    own_core = here.steps[3][0]
    own_chip = here.chip(home)
    own = here.worker(home)

    barrier = pltpu.get_barrier_semaphore()
    partners = COLUMN + DIRECT + SIDES + ENDS
    for offset in partners:
        here.signal(barrier, offset)

    order = PASSED + COLUMN + DIRECT + LATE + [home]
    loads = []
    for slot, offset in enumerate(order):
        rows = pl.ds(pl.multiple_of(here.worker(offset) * ROWS, ROWS), ROWS)
        load = pltpu.make_async_copy(gradients_ref.at[rows], full.at[slot], load_sem.at[slot])
        load.start()
        loads.append(load)
    fetch = pltpu.make_async_copy(neighbours_hbm, neighbours_ref, load_sem.at[WORKERS])
    fetch.start()

    def start(slot):
        offset = order[slot]
        if offset in PASSED:
            here.send(hi.at[slot], passing.at[slot], over_send, pass_recv.at[slot], ACROSS)
        elif offset in DIRECT:
            here.send(hi.at[slot], got.at[own], over_send, hi_recv, offset)
        elif offset in COLUMN:
            here.send(hi.at[slot], got.at[own], hi_send, hi_recv, offset)

    for slot, offset in enumerate(order):
        loads[slot].wait()
        value = full[slot]
        high = value.astype(jnp.bfloat16)
        low = (value - high.astype(jnp.float32)).astype(jnp.bfloat16)
        if offset == home:
            got[own] = high
        else:
            hi[slot] = high
        if offset[3] == 0:
            lo[own_core, here.chip(offset)] = low
        else:
            lo_away[here.chip(offset)] = low
        if slot == 1:
            pl.semaphore_wait(barrier, len(partners))
            for ready in range(1 + 1):
                start(ready)
        if slot > 1:
            start(slot)

    for offset in SIDES + [ACROSS]:
        here.signal(plane_in, offset)
    here.send(lo_away, lo.at[own_core], lo_send.at[0], lo_recv.at[0], PAIR)

    fetch.wait()
    winner = winner_ref[0]
    row = lax.broadcasted_iota(jnp.int32, (WORKERS, ROWS), 0)
    column = lax.broadcasted_iota(jnp.int32, (WORKERS, ROWS), 1) // 16
    counts = jnp.zeros((WORKERS, ROWS), jnp.float32)
    for entry in range(neighbours_ref.shape[1]):
        counts += (neighbours_ref[:, entry : entry + 1] == column).astype(jnp.float32)

    wait_bytes(lo_away, lo_recv.at[0])
    lo_mine[...] = lo[lax.rem(winner, 2)]

    pl.semaphore_wait(plane_in, len(SIDES) + 1)
    for slot, offset in enumerate(order):
        if offset in LATE:
            here.send(hi.at[slot], got.at[own], over_send, hi_recv, offset)
    across = here.worker(ACROSS)
    for slot in range(max(ROUNDS, len(PASSED))):
        if slot < ROUNDS:
            for offset in ENDS:
                here.signal(line_in.at[slot], offset)
        if slot < len(PASSED):
            _, dy, _, dc = PASSED[slot]
            wait_bytes(passing.at[slot], pass_recv.at[slot])
            here.send(passing.at[slot], got.at[across], hi_send, hi_recv, (0, dy, 0, dc))
        if slot < ROUNDS:
            pl.semaphore_wait(line_in.at[slot], len(ENDS))

    wait_bytes(hi.at[pl.ds(0, 8)], over_send)
    for offset in LOW_ACROSS:
        here.send(
            lo_mine.at[here.chip(offset)],
            lo_got.at[own_chip],
            lo_send.at[1],
            lo_recv.at[1],
            offset,
        )
    wait_bytes(got.at[pl.ds(0, 15)], hi_recv)
    lo_got[own_chip] = lo_mine[own_chip]

    for offset in LOW_COLUMN:
        here.send(
            lo_mine.at[here.chip(offset)],
            lo_got.at[own_chip],
            lo_send.at[1],
            lo_recv.at[1],
            offset,
        )
    parts = [got[:, pl.ds(step * 16, 16), :].reshape(ROWS, LANES) for step in range(ROWS // 16)]
    block = jnp.concatenate(parts, axis=1)
    total = lax.dot_general(
        block, block, (((1,), (1,)), ((), ())), preferred_element_type=jnp.float32
    )
    sublane = lax.broadcasted_iota(jnp.int32, (ROWS, ROWS), 0)
    lane = lax.broadcasted_iota(jnp.int32, (ROWS, ROWS), 1)
    total = jnp.where(lax.rem(sublane, 16) == lax.rem(lane, 16), total, 0.0)
    total = jnp.sum(total.reshape(WORKERS, 16, ROWS), axis=1)
    diagonal = jnp.where(row == column, total, 0.0)
    squares = jnp.sum(diagonal, axis=0, keepdims=True)
    own_counts = jnp.sum(counts, axis=1, keepdims=True) * (1.0 / 16.0)
    partial = counts * (squares - 2.0 * total) + own_counts * diagonal
    partial = jnp.sum(partial, axis=1, keepdims=True)
    place = lax.broadcasted_iota(jnp.int32, (WORKERS, LANES), 1)
    partial = jnp.where(row[:, :LANES] == place, partial, 0.0)
    own_sum[...] = jnp.sum(partial, axis=0, keepdims=True)

    here.send(own_sum, pair_got, sum_send.at[0], sum_recv.at[0], PAIR)
    wait_bytes(pair_got, sum_recv.at[0])
    pair_sum[...] = own_sum[...] + pair_got[...]
    for step, offset in enumerate(SLICE):
        here.send(pair_sum, sums_got.at[step], sum_send.at[1], sum_recv.at[1], offset)

    wait_bytes(lo_got.at[pl.ds(0, 7)], lo_recv.at[1])
    aggregate_ref[...] = got[winner].astype(jnp.float32) + lo_got[winner // 2].astype(jnp.float32)

    wait_bytes(sums_got, sum_recv.at[1])
    scores = pair_sum[...] + jnp.sum(sums_got[...], axis=0)
    scores_ref[...] = scores[0, :WORKERS] / jnp.float32(total_entries)

    wait_bytes(got.at[pl.ds(0, len(COLUMN) + len(PASSED))], hi_send)
    wait_bytes(lo_away, lo_send.at[0])
    wait_bytes(lo_got.at[pl.ds(0, 7)], lo_send.at[1])
    wait_bytes(pair_got, sum_send.at[0])
    wait_bytes(sums_got, sum_send.at[1])


def finish(scores_ref, block_ref, scores_hbm, block_hbm, sem):
    copies = (
        pltpu.make_async_copy(scores_ref, scores_hbm, sem.at[0]),
        pltpu.make_async_copy(block_ref, block_hbm, sem.at[1]),
    )
    for copy in copies:
        copy.start()
    for copy in copies:
        copy.wait()


def body(gradients, neighbours, winner):
    length = gradients.shape[1]
    total_entries = neighbours.shape[1] * length * lax.axis_size(MP)
    bf16, f32 = jnp.bfloat16, jnp.float32
    out_shape = (
        jax.ShapeDtypeStruct((WORKERS,), f32),
        jax.ShapeDtypeStruct((ROWS, LANES), f32),
    )
    scores, aggregate = pl.pallas_call(
        functools.partial(kernel, total_entries),
        out_shape=out_shape,
        in_specs=[
            pl.BlockSpec(memory_space=pltpu.SMEM),
            pl.BlockSpec(memory_space=pltpu.HBM),
            pl.BlockSpec(memory_space=pltpu.HBM),
        ],
        out_specs=(pl.BlockSpec(memory_space=pltpu.VMEM),) * 2,
        scratch_shapes=[
            pltpu.VMEM((WORKERS, ROWS, LANES), f32),
            pltpu.VMEM((15, ROWS, LANES), bf16),
            pltpu.VMEM((len(PASSED), ROWS, LANES), bf16),
            pltpu.VMEM((WORKERS, ROWS, LANES), bf16),
            pltpu.VMEM((2, 8, ROWS, LANES), bf16),
            pltpu.VMEM((8, ROWS, LANES), bf16),
            pltpu.VMEM((8, ROWS, LANES), bf16),
            pltpu.VMEM((8, ROWS, LANES), bf16),
            pltpu.VMEM((1, LANES), f32),
            pltpu.VMEM((1, LANES), f32),
            pltpu.VMEM((1, LANES), f32),
            pltpu.VMEM((len(SLICE), 1, LANES), f32),
            pltpu.VMEM(neighbours.shape, jnp.int32),
            pltpu.SemaphoreType.DMA((WORKERS + 1,)),
            pltpu.SemaphoreType.DMA,
            pltpu.SemaphoreType.DMA,
            pltpu.SemaphoreType.DMA,
            pltpu.SemaphoreType.DMA((len(PASSED),)),
            pltpu.SemaphoreType.DMA((2,)),
            pltpu.SemaphoreType.DMA((2,)),
            pltpu.SemaphoreType.DMA((2,)),
            pltpu.SemaphoreType.DMA((2,)),
            pltpu.SemaphoreType.REGULAR,
            pltpu.SemaphoreType.REGULAR((ROUNDS,)),
        ],
        compiler_params=pltpu.CompilerParams(
            collective_id=0, has_side_effects=True, vmem_limit_bytes=24 << 20
        ),
        name="krum",
    )(
        winner,
        pltpu.with_memory_space_constraint(neighbours, pltpu.HBM),
        pltpu.with_memory_space_constraint(
            gradients.reshape(length // LANES, LANES), pltpu.HBM
        ),
    )
    scores, aggregate = pl.pallas_call(
        finish,
        out_shape=out_shape,
        in_specs=[pl.BlockSpec(memory_space=pltpu.VMEM)] * 2,
        out_specs=(pl.BlockSpec(memory_space=pltpu.HBM),) * 2,
        scratch_shapes=[pltpu.SemaphoreType.DMA((2,))],
        compiler_params=pltpu.CompilerParams(vmem_limit_bytes=1 << 20),
        name="finish",
    )(scores, aggregate)
    return scores, aggregate.reshape(-1)


def solution(mesh):
    split = Mesh(mesh.devices.reshape(4, 2, 2, 8, 2), AXES)
    in_specs = (P(WORKER, MP), P(), P())
    out_specs = (P(), P(MP_WORKER))
    return jax.shard_map(body, mesh=split, in_specs=in_specs, out_specs=out_specs, check_vma=False)
```

```python
import functools

import jax
import jax.numpy as jnp
from jax import lax
from jax.experimental import pallas as pl
from jax.experimental.pallas import tpu as pltpu
from jax.sharding import Mesh
from jax.sharding import PartitionSpec as P

AXES = ("y", "xh", "c", "z", "xl")
WORKER = ("y", "xh", "c")
MP = ("z", "xl")
MP_WORKER = ("z", "xl", "y", "xh", "c")
MESH = pl.DeviceIdType.MESH

WORKERS = 16
ROWS = 256
LANES = 128

PAIR = (0, 0, 0, 1)
ACROSS = (2, 0, 0, 0)
PASSED = [(2, dy, 0, dc) for dy, dc in ((2, 0), (2, 1),)]
LATE = [(2, dy, 0, dc) for dy, dc in ((1, 0), (3, 0), (1, 1), (3, 1),)]
DIRECT = [(2, 0, 0, 1), ACROSS]
COLUMN = [(0, dy, 0, dc) for dy in (2, 1, 3) for dc in (0, 1)] + [PAIR]
LOW_ACROSS = [(2, dy, 0, 0) for dy in (2, 1, 3, 0)]
LOW_COLUMN = [(0, dy, 0, 0) for dy in (2, 1, 3)]
SIDES = [(1, 0, 0, 0), (3, 0, 0, 0)]
ENDS = [(0, 0, 1, 0), (0, 0, 7, 0)]
ROUNDS = 4
BEFORE = 2
SLICE = [
    (dx, dy, dz, 0)
    for dx, dy, dz in sorted(
        ((a, b, d) for a in range(4) for b in range(4) for d in range(8)),
        key=lambda p: -(min(p[0], 4 - p[0]) + min(p[1], 4 - p[1]) + min(p[2], 8 - p[2])),
    )
    if (dx, dy, dz) != (0, 0, 0)
]


class Place:
    def __init__(self):
        x = lax.axis_index("xh") * 2 + lax.axis_index("xl")
        own = (x, lax.axis_index("y"), lax.axis_index("z"), lax.axis_index("c"))
        self.steps = [
            [value] + [lax.rem(value + step, size) for step in range(1, size)]
            for value, size in zip(own, (4, 4, 8, 2))
        ]
        self.x_hi = [x // 2 for x in self.steps[0]]
        self.x_lo = [lax.rem(x, 2) for x in self.steps[0]]

    def device(self, offset):
        dx, dy, dz, dc = offset
        _, y, z, c = self.steps
        return {"y": y[dy], "xh": self.x_hi[dx], "c": c[dc], "z": z[dz], "xl": self.x_lo[dx]}

    def chip(self, offset):
        return self.steps[1][offset[1]] * 2 + self.x_hi[offset[0]]

    def worker(self, offset):
        return self.chip(offset) * 2 + self.steps[3][offset[3]]

    def signal(self, sem, offset):
        pl.semaphore_signal(sem, inc=1, device_id=self.device(offset), device_id_type=MESH)

    def send(self, src, dst, send_sem, recv_sem, offset):
        pltpu.make_async_remote_copy(
            src_ref=src,
            dst_ref=dst,
            send_sem=send_sem,
            recv_sem=recv_sem,
            device_id=self.device(offset),
            device_id_type=MESH,
        ).start()


def wait_bytes(ref, sem):
    pltpu.make_async_copy(ref, ref, sem).wait()


def kernel(
    total_entries,
    winner_ref,
    neighbours_hbm,
    gradients_ref,
    scores_ref,
    aggregate_ref,
    full,
    hi,
    passing,
    got,
    lo,
    lo_away,
    lo_mine,
    lo_got,
    own_sum,
    pair_got,
    pair_sum,
    sums_got,
    neighbours_ref,
    load_sem,
    hi_send,
    over_send,
    hi_recv,
    pass_recv,
    lo_send,
    lo_recv,
    sum_send,
    sum_recv,
    plane_in,
    line_in,
):
    here = Place()
    home = (0, 0, 0, 0)
    own_core = here.steps[3][0]
    own_chip = here.chip(home)
    own = here.worker(home)

    barrier = pltpu.get_barrier_semaphore()
    partners = COLUMN + DIRECT + SIDES + ENDS
    for offset in partners:
        here.signal(barrier, offset)

    order = PASSED + COLUMN + DIRECT + LATE + [home]
    loads = []
    for slot, offset in enumerate(order):
        rows = pl.ds(pl.multiple_of(here.worker(offset) * ROWS, ROWS), ROWS)
        load = pltpu.make_async_copy(gradients_ref.at[rows], full.at[slot], load_sem.at[slot])
        load.start()
        loads.append(load)
    fetch = pltpu.make_async_copy(neighbours_hbm, neighbours_ref, load_sem.at[WORKERS])
    fetch.start()

    def start(slot):
        offset = order[slot]
        if offset in PASSED:
            here.send(hi.at[slot], passing.at[slot], over_send, pass_recv.at[slot], ACROSS)
        elif offset in DIRECT:
            here.send(hi.at[slot], got.at[own], over_send, hi_recv, offset)
        elif offset in COLUMN:
            here.send(hi.at[slot], got.at[own], hi_send, hi_recv, offset)

    for slot, offset in enumerate(order):
        loads[slot].wait()
        value = full[slot]
        high = value.astype(jnp.bfloat16)
        low = (value - high.astype(jnp.float32)).astype(jnp.bfloat16)
        if offset == home:
            got[own] = high
        else:
            hi[slot] = high
        if offset[3] == 0:
            lo[own_core, here.chip(offset)] = low
        else:
            lo_away[here.chip(offset)] = low
        if slot == BEFORE:
            pl.semaphore_wait(barrier, len(partners))
            for first in range(slot - 1):
                start(first)
        if slot >= BEFORE:
            start(slot - 1)

    for offset in SIDES + [ACROSS]:
        here.signal(plane_in, offset)
    here.send(lo_away, lo.at[own_core], lo_send.at[0], lo_recv.at[0], PAIR)

    fetch.wait()
    winner = winner_ref[0]
    row = lax.broadcasted_iota(jnp.int32, (WORKERS, ROWS), 0)
    column = lax.broadcasted_iota(jnp.int32, (WORKERS, ROWS), 1) // 16
    counts = jnp.zeros((WORKERS, ROWS), jnp.float32)
    for entry in range(neighbours_ref.shape[1]):
        counts += (neighbours_ref[:, entry : entry + 1] == column).astype(jnp.float32)

    wait_bytes(lo_away, lo_recv.at[0])
    lo_mine[...] = lo[lax.rem(winner, 2)]

    pl.semaphore_wait(plane_in, len(SIDES) + 1)
    for slot, offset in enumerate(order):
        if offset in LATE:
            here.send(hi.at[slot], got.at[own], over_send, hi_recv, offset)
    across = here.worker(ACROSS)
    for slot in range(max(ROUNDS, len(PASSED))):
        if slot < ROUNDS:
            for offset in ENDS:
                here.signal(line_in.at[slot], offset)
        if slot < len(PASSED):
            _, dy, _, dc = PASSED[slot]
            wait_bytes(passing.at[slot], pass_recv.at[slot])
            here.send(passing.at[slot], got.at[across], hi_send, hi_recv, (0, dy, 0, dc))
        if slot < ROUNDS:
            pl.semaphore_wait(line_in.at[slot], len(ENDS))

    wait_bytes(hi.at[pl.ds(0, 8)], over_send)
    for offset in LOW_ACROSS:
        here.send(
            lo_mine.at[here.chip(offset)],
            lo_got.at[own_chip],
            lo_send.at[1],
            lo_recv.at[1],
            offset,
        )
    wait_bytes(got.at[pl.ds(0, 15)], hi_recv)
    lo_got[own_chip] = lo_mine[own_chip]

    for offset in LOW_COLUMN:
        here.send(
            lo_mine.at[here.chip(offset)],
            lo_got.at[own_chip],
            lo_send.at[1],
            lo_recv.at[1],
            offset,
        )
    parts = [got[:, pl.ds(step * 16, 16), :].reshape(ROWS, LANES) for step in range(ROWS // 16)]
    block = jnp.concatenate(parts, axis=1)
    total = lax.dot_general(
        block, block, (((1,), (1,)), ((), ())), preferred_element_type=jnp.float32
    )
    sublane = lax.broadcasted_iota(jnp.int32, (ROWS, ROWS), 0)
    lane = lax.broadcasted_iota(jnp.int32, (ROWS, ROWS), 1)
    total = jnp.where(lax.rem(sublane, 16) == lax.rem(lane, 16), total, 0.0)
    total = jnp.sum(total.reshape(WORKERS, 16, ROWS), axis=1)
    diagonal = jnp.where(row == column, total, 0.0)
    squares = jnp.sum(diagonal, axis=0, keepdims=True)
    own_counts = jnp.sum(counts, axis=1, keepdims=True) * (1.0 / 16.0)
    partial = counts * (squares - 2.0 * total) + own_counts * diagonal
    partial = jnp.sum(partial, axis=1, keepdims=True)
    place = lax.broadcasted_iota(jnp.int32, (WORKERS, LANES), 1)
    partial = jnp.where(row[:, :LANES] == place, partial, 0.0)
    own_sum[...] = jnp.sum(partial, axis=0, keepdims=True)

    here.send(own_sum, pair_got, sum_send.at[0], sum_recv.at[0], PAIR)
    wait_bytes(pair_got, sum_recv.at[0])
    pair_sum[...] = own_sum[...] + pair_got[...]
    for step, offset in enumerate(SLICE):
        here.send(pair_sum, sums_got.at[step], sum_send.at[1], sum_recv.at[1], offset)

    wait_bytes(lo_got.at[pl.ds(0, 7)], lo_recv.at[1])
    aggregate_ref[...] = got[winner].astype(jnp.float32) + lo_got[winner // 2].astype(jnp.float32)

    wait_bytes(sums_got, sum_recv.at[1])
    scores = pair_sum[...] + jnp.sum(sums_got[...], axis=0)
    scores_ref[...] = scores[0, :WORKERS] / jnp.float32(total_entries)

    wait_bytes(got.at[pl.ds(0, len(COLUMN) + len(PASSED))], hi_send)
    wait_bytes(lo_away, lo_send.at[0])
    wait_bytes(lo_got.at[pl.ds(0, 7)], lo_send.at[1])
    wait_bytes(pair_got, sum_send.at[0])
    wait_bytes(sums_got, sum_send.at[1])


def finish(scores_ref, block_ref, scores_hbm, block_hbm, sem):
    copies = (
        pltpu.make_async_copy(scores_ref, scores_hbm, sem.at[0]),
        pltpu.make_async_copy(block_ref, block_hbm, sem.at[1]),
    )
    for copy in copies:
        copy.start()
    for copy in copies:
        copy.wait()


def body(gradients, neighbours, winner):
    length = gradients.shape[1]
    total_entries = neighbours.shape[1] * length * lax.axis_size(MP)
    bf16, f32 = jnp.bfloat16, jnp.float32
    out_shape = (
        jax.ShapeDtypeStruct((WORKERS,), f32),
        jax.ShapeDtypeStruct((ROWS, LANES), f32),
    )
    scores, aggregate = pl.pallas_call(
        functools.partial(kernel, total_entries),
        out_shape=out_shape,
        in_specs=[
            pl.BlockSpec(memory_space=pltpu.SMEM),
            pl.BlockSpec(memory_space=pltpu.HBM),
            pl.BlockSpec(memory_space=pltpu.HBM),
        ],
        out_specs=(pl.BlockSpec(memory_space=pltpu.VMEM),) * 2,
        scratch_shapes=[
            pltpu.VMEM((WORKERS, ROWS, LANES), f32),
            pltpu.VMEM((15, ROWS, LANES), bf16),
            pltpu.VMEM((len(PASSED), ROWS, LANES), bf16),
            pltpu.VMEM((WORKERS, ROWS, LANES), bf16),
            pltpu.VMEM((2, 8, ROWS, LANES), bf16),
            pltpu.VMEM((8, ROWS, LANES), bf16),
            pltpu.VMEM((8, ROWS, LANES), bf16),
            pltpu.VMEM((8, ROWS, LANES), bf16),
            pltpu.VMEM((1, LANES), f32),
            pltpu.VMEM((1, LANES), f32),
            pltpu.VMEM((1, LANES), f32),
            pltpu.VMEM((len(SLICE), 1, LANES), f32),
            pltpu.VMEM(neighbours.shape, jnp.int32),
            pltpu.SemaphoreType.DMA((WORKERS + 1,)),
            pltpu.SemaphoreType.DMA,
            pltpu.SemaphoreType.DMA,
            pltpu.SemaphoreType.DMA,
            pltpu.SemaphoreType.DMA((len(PASSED),)),
            pltpu.SemaphoreType.DMA((2,)),
            pltpu.SemaphoreType.DMA((2,)),
            pltpu.SemaphoreType.DMA((2,)),
            pltpu.SemaphoreType.DMA((2,)),
            pltpu.SemaphoreType.REGULAR,
            pltpu.SemaphoreType.REGULAR((ROUNDS,)),
        ],
        compiler_params=pltpu.CompilerParams(
            collective_id=0, has_side_effects=True, vmem_limit_bytes=24 << 20
        ),
        name="krum",
    )(
        winner,
        pltpu.with_memory_space_constraint(neighbours, pltpu.HBM),
        pltpu.with_memory_space_constraint(
            gradients.reshape(length // LANES, LANES), pltpu.HBM
        ),
    )
    scores, aggregate = pl.pallas_call(
        finish,
        out_shape=out_shape,
        in_specs=[pl.BlockSpec(memory_space=pltpu.VMEM)] * 2,
        out_specs=(pl.BlockSpec(memory_space=pltpu.HBM),) * 2,
        scratch_shapes=[pltpu.SemaphoreType.DMA((2,))],
        compiler_params=pltpu.CompilerParams(vmem_limit_bytes=1 << 20),
        name="finish",
    )(scores, aggregate)
    return scores, aggregate.reshape(-1)


def solution(mesh):
    split = Mesh(mesh.devices.reshape(4, 2, 2, 8, 2), AXES)
    in_specs = (P(WORKER, MP), P(), P())
    out_specs = (P(), P(MP_WORKER))
    return jax.shard_map(body, mesh=split, in_specs=in_specs, out_specs=out_specs, check_vma=False)
```
